512 devices in a mesh: clus: 16 (over x_lo, z), seq: 32 (over y, x_hi, core).
Axes of the slice: x: 4 (x_hi: 2, x_lo: 2; x = x_hi * 2 + x_lo), y: 8, z: 8, core: 2. Of those that a mesh axis runs over, the one named last changes fastest.
Arguments:
- embeddings: bfloat16 [131072, 768], P(('clus', 'seq')), parts along dimension 0, may hold values from -1 to 1, as said below
- doc_order: int32 [512, 256], P(('clus', 'seq')), parts along dimension 0, may hold values from 0 to 255, each once within a row
Outputs:
- prior_max: float32 [131072], P(('clus', 'seq')), parts along dimension 0
- later_max: float32 [131072], P(('clus', 'seq')), parts along dimension 0
The draws below stay inside these ranges and needn't reach their ends.
There are 16 independent parts, one for each index of `clus`. The reference program is written for one: setup_inputs(seed, part) draws one part's arguments, and reference() takes and returns one part's arrays. A program takes and returns all parts, laid end to end along the dimension named above; each array names one. Nothing has to cross between parts.
Inputs may be any that keep to these rules, and one draw needn't show every extreme that they name: `embeddings`: each row has unit Euclidean length up to bfloat16 rounding. `doc_order`: each row is a permutation of 0 to 255.
All inputs are finite; a program needn't handle non-finite values.
Results may differ from the reference program's by a relative error of at most 0.0003.
Values may be sent and summed in bfloat16 or wider, within the bound.
A program may use at most 64 MiB of HBM per device.

```python
import jax
import jax.numpy as jnp
from jax import lax

D = 768
BLK = 256
BLOCKS = 32
ROWS = 8192


def draw_embeddings(key, part):
    key_noise = jax.random.fold_in(key, 11)
    key_center = jax.random.fold_in(key, 12)
    key_weight = jax.random.fold_in(key, 13)
    key_assign = jax.random.fold_in(key, 14)
    center_count = 32
    assign = jax.random.randint(key_assign, (ROWS,), 0, center_count)
    centers = jax.random.normal(key_center, (center_count, D), jnp.float32)
    noise = jax.random.normal(key_noise, (ROWS, D), jnp.float32)
    weight = jax.random.uniform(key_weight, (ROWS,), jnp.float32, 0.6, 1.6)
    chosen = centers[assign]
    mixed = noise + weight[:, None] * chosen
    length = jnp.sqrt(jnp.sum(mixed * mixed, axis=1, keepdims=True))
    return (mixed / length).astype(jnp.bfloat16)


def setup_inputs(seed: int = 0, part: int = 0) -> dict:
    keys = jax.random.split(jax.random.key(seed), 3)
    own_keys = jax.random.split(jax.random.fold_in(keys[2], part), 3)
    embeddings = draw_embeddings(jax.random.fold_in(jax.random.fold_in(keys[2], part), 71), part)
    doc_order = jax.vmap(lambda own: jax.random.permutation(own, BLK))(jax.random.split(own_keys[1], BLOCKS)).reshape((BLOCKS, BLK)).astype(jnp.int32)
    return dict(embeddings=embeddings, doc_order=doc_order)


def reference(embeddings, doc_order):
    members = embeddings.astype(jnp.float32)
    ranking = doc_order.reshape(ROWS)
    column_block = (jnp.arange(ROWS, dtype=jnp.int32) // BLK).astype(jnp.int32)

    def one_block(block_index):
        rows_here = lax.dynamic_slice_in_dim(members, (block_index * BLK).astype(jnp.int32), BLK, 0)
        rank_here = lax.dynamic_slice_in_dim(ranking, (block_index * BLK).astype(jnp.int32), BLK, 0)
        similar = jnp.dot(rows_here, members.T, precision=lax.Precision.HIGHEST, preferred_element_type=jnp.float32)
        same_block = (column_block == block_index)[None, :]
        before = (column_block < block_index)[None, :] | (same_block & (ranking[None, :] < rank_here[:, None]))
        after = (column_block > block_index)[None, :] | (same_block & (ranking[None, :] > rank_here[:, None]))
        prior_part = jnp.max(jnp.where(before, similar, jnp.float32(-1.0)), axis=1)
        later_part = jnp.max(jnp.where(after, similar, jnp.float32(-1.0)), axis=1)
        return prior_part, later_part

    prior_parts, later_parts = lax.map(one_block, jnp.arange(BLOCKS, dtype=jnp.int32))
    return prior_parts.reshape(ROWS), later_parts.reshape(ROWS)
```

```python
import jax
import jax.numpy as jnp
from jax import lax
from jax.experimental import pallas as pl
from jax.experimental.pallas import tpu as pltpu
from jax.sharding import PartitionSpec as P

MESH = pl.DeviceIdType.MESH
CHUNKS = 4
YS = 8


def sims(left, right):
    return lax.dot_general(left, right, (((1,), (1,)), ((), ())), preferred_element_type=jnp.float32)


def colmax(s):
    return jnp.max(s, axis=0, keepdims=True)


def lanes(s):
    out = s[:, :128]
    for j in range(1, s.shape[1] // 128):
        out = jnp.maximum(out, s[:, j * 128 : (j + 1) * 128])
    return out


def flip(r):
    return jnp.max(jnp.transpose(r), axis=0, keepdims=True)


def kernel(emb, order, out, own, m1, m2, pc, e, own2, rank, msg_out, msg_in,
           csem, s_ring, r_ring, s_sib, r_sib, s_msg, r_msg):
    clus = lax.axis_index("clus")
    seq = lax.axis_index("seq")
    y, h, c = seq // 4, (seq // 2) % 2, seq % 2

    def dev(dy, hh, cc):
        return (clus, ((y + dy + YS) % YS) * 4 + hh * 2 + cc)

    up, down = dev(1, h, c), dev(-1, h, c)
    across, sib = dev(0, 1 - h, c), dev(0, h, 1 - c)
    rows = own.shape[0] // CHUNKS

    def part(k):
        return pl.ds(k * rows, rows)

    load = pltpu.make_async_copy(emb, own, csem.at[0])
    load_rank = pltpu.make_async_copy(order, rank, csem.at[1])
    load.start()
    load_rank.start()
    barrier = pltpu.get_barrier_semaphore()
    for d in (up, down, across, sib):
        pl.semaphore_signal(barrier, inc=1, device_id=d, device_id_type=MESH)
    pl.semaphore_wait(barrier, 4)
    load.wait()
    load_rank.wait()

    sent = []

    def send(src, dst, s, r, d):
        copy = pltpu.make_async_remote_copy(
            src_ref=src, dst_ref=dst, send_sem=s, recv_sem=r, device_id=d, device_id_type=MESH
        )
        sent.append(copy)
        return copy

    ring = lambda i, k: (s_ring.at[i, k], r_ring.at[i, k])
    near = lambda i, k: (s_sib.at[i, k], r_sib.at[i, k])
    c_m1 = [send(own.at[part(k)], m1.at[part(k)], *ring(0, k), up) for k in range(CHUNKS)]
    c_p1 = [send(own.at[part(k)], pc.at[0, c, part(k)], *ring(1, k), down) for k in range(CHUNKS)]
    c_m2 = [send(m1.at[part(k)], m2.at[part(k)], *ring(2, k), up) for k in range(CHUNKS)]
    which = ((y + 7) % YS) // 4
    c_e = [send(pc.at[which, c, part(k)], e.at[c, part(k)], *ring(3, k), down) for k in range(CHUNKS)]
    c_c1 = [send(pc.at[0, c, part(k)], pc.at[1, c, part(k)], *ring(4, k), across) for k in range(CHUNKS)]
    c_own = send(own, own2, *near(0, 0), sib)
    n_p1 = [send(pc.at[0, c, part(k)], pc.at[0, c, part(k)], *near(1, k), sib) for k in range(CHUNKS)]
    n_c1 = [send(pc.at[1, c, part(k)], pc.at[1, c, part(k)], *near(2, k), sib) for k in range(CHUNKS)]
    n_e = [send(e.at[c, part(k)], e.at[c, part(k)], *near(3, k), sib) for k in range(CHUNKS)]

    for k in range(CHUNKS):
        c_m1[k].start()
        c_p1[k].start()
    c_own.start()

    neg = jnp.float32(-1.0)
    rank_cols = jnp.broadcast_to(rank[...].astype(jnp.float32), (256, 256))
    rank_rows = jnp.transpose(rank_cols)
    s = sims(own[...], own[...])
    prior0 = colmax(jnp.where(rank_rows < rank_cols, s, neg))
    later0 = colmax(jnp.where(rank_rows > rank_cols, s, neg))

    for k in range(CHUNKS):
        c_m1[k].wait_recv()
        c_m2[k].start()
        c_p1[k].wait_recv()
        c_c1[k].start()
        n_p1[k].start()
        if k >= 1:
            c_c1[k - 1].wait_recv()
            c_e[k - 1].start()
            n_c1[k - 1].start()
    k = CHUNKS - 1
    c_c1[k].wait_recv()
    c_e[k].start()
    n_c1[k].start()

    c_own.wait_recv()
    s01 = colmax(sims(own2[...], own[...]))
    prior0 = jnp.maximum(prior0, jnp.where(c == 1, s01, neg))
    later0 = jnp.maximum(later0, jnp.where(c == 0, s01, neg))

    for k in range(CHUNKS):
        n_p1[k].wait_recv()

    def meet(a, kind, col):
        r = None
        for j in range(2):
            s = sims(a, pc[kind, j])
            col.append(colmax(s))
            r = lanes(s) if r is None else jnp.maximum(r, lanes(s))
        return r

    col0, col1, col2 = [], [], []
    r0 = meet(own[...], 0, col0)
    r1 = meet(m1[...], 0, col1)
    for k in range(CHUNKS):
        n_c1[k].wait_recv()
    r0 = jnp.maximum(r0, meet(own[...], 1, col0))
    r1 = jnp.maximum(r1, meet(m1[...], 1, col1))
    other = (c + h) % 2
    pblk, cblk = pc[0, c], pc[1, other]
    pcol = colmax(sims(cblk, pblk))
    ccol = colmax(sims(pblk, cblk))
    r0, r1 = flip(r0), flip(r1)

    for k in range(CHUNKS):
        c_e[k].wait_recv()
        n_e[k].start()
    for k in range(CHUNKS):
        c_m2[k].wait_recv()
    r2 = meet(m2[...], 0, col2)
    r2 = flip(jnp.maximum(r2, meet(m2[...], 1, col2)))
    ecol, re = [], None
    for k in range(CHUNKS):
        n_e[k].wait_recv()
    for j in range(2):
        s = sims(m2[...], e[j])
        ecol.append(colmax(s))
        re = lanes(s) if re is None else jnp.maximum(re, lanes(s))
    re = flip(re)

    at = lambda dy: (y + dy + YS) % YS
    first0, first1, first2, first2e = at(0) < at(1), at(-1) < at(1), at(-2) < at(1), at(-2) < at(2)

    def pick(flag, v):
        return jnp.where(flag, v, neg)

    def top(*vs):
        o = vs[0]
        for v in vs[1:]:
            o = jnp.maximum(o, v)
        return o

    prior0 = top(prior0, pick(~first0, r0))
    later0 = top(later0, pick(first0, r0))

    def put(i, prior, later):
        msg_out[i, 0:1, :] = jnp.maximum(prior, neg)
        msg_out[i, 1:2, :] = jnp.maximum(later, neg)

    put(0, pick(~first1, r1), pick(first1, r1))
    put(1, top(pick(~first2, r2), pick(~first2e, re)), top(pick(first2, r2), pick(first2e, re)))
    for j in range(2):
        x = [col0[j], col1[j], col2[j]]
        mine = pick(c == j, pcol)
        put(2 + j,
            top(pick(h == 1, mine), *[pick(f, v) for f, v in zip((first0, first1, first2), x)]),
            top(pick(h == 0, mine), *[pick(~f, v) for f, v in zip((first0, first1, first2), x)]))
        x = [col0[2 + j], col1[2 + j], col2[2 + j]]
        mine = pick(other == j, ccol)
        put(4 + j,
            top(pick(h == 0, mine), *[pick(f, v) for f, v in zip((first0, first1, first2), x)]),
            top(pick(h == 1, mine), *[pick(~f, v) for f, v in zip((first0, first1, first2), x)]))
        put(6 + j, pick(first2e, ecol[j]), pick(~first2e, ecol[j]))

    he = (h + y // 4) % 2
    results = []
    for i, slot, d in [
        (0, 0, dev(-1, h, c)), (1, 1, dev(-2, h, c)),
        (2, 2 + c, dev(1, h, 0)), (3, 2 + c, dev(1, h, 1)),
        (4, 4 + c, dev(1, 1 - h, 0)), (5, 4 + c, dev(1, 1 - h, 1)),
        (6, 6 + c, dev(2, he, 0)), (7, 6 + c, dev(2, he, 1)),
    ]:
        copy = send(msg_out.at[i], msg_in.at[slot], s_msg.at[i], r_msg.at[slot], d)
        copy.start()
        results.append(copy)
    for i in range(8):
        pltpu.make_async_remote_copy(
            src_ref=msg_out.at[i], dst_ref=msg_in.at[i], send_sem=s_msg.at[i], recv_sem=r_msg.at[i],
            device_id=up, device_id_type=MESH,
        ).wait_recv()
    got = msg_in[...]
    best = jnp.max(got, axis=0)
    out[...] = jnp.maximum(best, jnp.concatenate([prior0, later0], axis=0))
    for copy in sent:
        copy.wait_send()


def per_device(embeddings, doc_order):
    rows, width = embeddings.shape
    block = (rows, width)
    vm = lambda *lead: pltpu.VMEM((*lead, *block), jnp.bfloat16)
    dma = lambda *n: pltpu.SemaphoreType.DMA(n)
    both = pl.pallas_call(
        kernel,
        name="dedup",
        out_shape=jax.ShapeDtypeStruct((2, rows), jnp.float32),
        in_specs=[pl.BlockSpec(memory_space=pl.ANY)] * 2,
        out_specs=pl.BlockSpec(memory_space=pltpu.VMEM),
        scratch_shapes=[
            vm(), vm(), vm(), vm(2, 2), vm(2), vm(),
            pltpu.VMEM((1, rows), jnp.int32),
            pltpu.VMEM((8, 2, rows), jnp.float32),
            pltpu.VMEM((8, 2, rows), jnp.float32),
            dma(2), dma(5, CHUNKS), dma(5, CHUNKS), dma(4, CHUNKS), dma(4, CHUNKS), dma(8), dma(8),
        ],
        compiler_params=pltpu.CompilerParams(
            collective_id=0, has_side_effects=True, vmem_limit_bytes=32 * 1024 * 1024
        ),
    )(embeddings, doc_order)
    return both[0], both[1]


def solution(mesh):
    return jax.shard_map(
        per_device,
        mesh=mesh,
        in_specs=(P(("clus", "seq"), None), P(("clus", "seq"), None)),
        out_specs=(P(("clus", "seq")), P(("clus", "seq"))),
        check_vma=False,
    )
```

```python
import jax
import jax.numpy as jnp
from jax import lax
from jax.experimental import pallas as pl
from jax.experimental.pallas import tpu as pltpu
from jax.sharding import PartitionSpec as P

MESH = pl.DeviceIdType.MESH
CHUNKS = 8
LAG = CHUNKS // 2
OPEN = 2
DELTA = 3
YS = 8


def sims(left, right):
    return lax.dot_general(left, right, (((1,), (1,)), ((), ())), preferred_element_type=jnp.float32)


def colmax(s):
    return jnp.max(s, axis=0, keepdims=True)


def lanes(s):
    out = s[:, :128]
    for j in range(1, s.shape[1] // 128):
        out = jnp.maximum(out, s[:, j * 128 : (j + 1) * 128])
    return out


def flip(r):
    return jnp.max(jnp.transpose(r), axis=0, keepdims=True)


def kernel(emb, order, out, own, m1, m2, pc, e, own2, rank, msg_out,
           hello, csem, s_sem, r_ring, r_all):
    clus = lax.axis_index("clus")
    seq = lax.axis_index("seq")
    y, h, c = seq // 4, (seq // 2) % 2, seq % 2

    def dev(dy, hh, cc):
        return (clus, ((y + dy + YS) % YS) * 4 + hh * 2 + cc)

    up, down = dev(1, h, c), dev(-1, h, c)
    across, sib = dev(0, 1 - h, c), dev(0, h, 1 - c)
    rows = own.shape[0] // CHUNKS

    def part(k):
        return pl.ds(k * rows, rows)

    even = (y + h + c) % 2 == 0
    odd = jnp.logical_not(even)
    no = jnp.logical_not
    corner = (clus == 0) & (c == 0)
    late_m1 = corner & (h == 0) & (y == 1)
    late_p1 = corner & (h == 0) & (y == YS - 1)
    late_c1 = corner & (h == 1) & ((y == 0) | (y == YS - 1))

    def signal(sem, *devices):
        for d in devices:
            pl.semaphore_signal(sem, inc=1, device_id=d, device_id_type=MESH)

    barrier = pltpu.get_barrier_semaphore()
    load = pltpu.make_async_copy(emb, own, csem.at[0])
    load_rank = pltpu.make_async_copy(order, rank, csem.at[1])
    load.start()
    load_rank.start()
    pl.when(even)(lambda: signal(barrier, across, sib))
    pl.when(odd)(lambda: signal(barrier, up, down))

    @pl.when(even)
    def _():
        pl.semaphore_wait(barrier, 2)
        signal(hello.at[0], down)
        signal(hello.at[1], up)

    load.wait()

    def copy(src, dst, stream, r, d):
        return pltpu.make_async_remote_copy(
            src_ref=src, dst_ref=dst, send_sem=s_sem.at[stream], recv_sem=r, device_id=d, device_id_type=MESH
        )

    which = ((y + 1) % YS) // 4
    every = range(CHUNKS)
    c_m1 = [copy(own.at[part(k)], m1.at[part(k)], 0, r_ring.at[0, k], up) for k in every]
    c_p1 = [copy(own.at[part(k)], pc.at[0, c, part(k)], 1, r_ring.at[1, k], down) for k in every]
    c_m2 = [copy(m1.at[part(k)], m2.at[part(k)], 2, r_all.at[0], up) for k in every]
    c_e = [copy(pc.at[which, c, part(k)], e.at[c, part(k)], 3, r_ring.at[3, k], down) for k in every]
    c_c1 = [copy(pc.at[0, c, part(k)], pc.at[1, c, part(k)], 4, r_ring.at[2, k], across) for k in every]
    c_own = copy(own, own2, 5, r_all.at[1], sib)
    n_p1 = [copy(pc.at[0, c, part(k)], pc.at[0, c, part(k)], 6, r_all.at[2], sib) for k in every]
    n_c1 = [copy(pc.at[1, c, part(k)], pc.at[1, c, part(k)], 7, r_all.at[3], sib) for k in every]
    n_e = [copy(e.at[c, part(k)], e.at[c, part(k)], 8, r_all.at[4], sib) for k in every]

    def take_all(i, dst):
        copy(own, dst, 0, r_all.at[i], up).wait_recv()

    def when(flag, *copies):
        @pl.when(flag)
        def _():
            for one in copies:
                one.start()

    when(even, *[one for pair in zip(c_m1, c_p1) for one in pair])

    def open_up():
        pl.semaphore_wait(hello.at[0], 1)
        for one in c_m1:
            one.start()

    def open_down():
        pl.semaphore_wait(hello.at[1], 1)
        for one in c_p1:
            one.start()

    @pl.when(odd & (y < YS // 2))
    def _():
        open_up()
        open_down()

    @pl.when(odd & (y >= YS // 2))
    def _():
        open_down()
        open_up()

    load_rank.wait()

    neg = jnp.float32(-1.0)
    rank_cols = jnp.broadcast_to(rank[...].astype(jnp.float32), (256, 256))
    rank_rows = jnp.transpose(rank_cols)
    s = sims(own[...], own[...])
    prior0 = colmax(jnp.where(rank_rows < rank_cols, s, neg))
    later0 = colmax(jnp.where(rank_rows > rank_cols, s, neg))

    @pl.when(odd)
    def _():
        pl.semaphore_wait(barrier, 2)
        signal(hello.at[2], across)
        signal(hello.at[3], sib)

    pl.when(even)(lambda: pl.semaphore_wait(hello.at[3], 1))
    c_own.start()

    def take_m1(k):
        c_m1[k].wait_recv()
        c_m2[k].start()

    def take_p1(k):
        c_p1[k].wait_recv()
        if k < OPEN:
            when(odd, c_c1[k])
        else:
            c_c1[k].start()
        when(which == 0, c_e[k])
        n_p1[k].start()

    def take_c1(k):
        c_c1[k].wait_recv()
        when(which == 1, c_e[k])
        n_c1[k].start()

    def turn(late, take, k):
        if 0 <= k < CHUNKS:
            pl.when(no(late))(lambda: take(k))
        if 0 <= k - DELTA < CHUNKS:
            pl.when(late)(lambda: take(k - DELTA))

    for k in range(CHUNKS + LAG + DELTA):
        if k == OPEN:
            pl.when(even)(lambda: pl.semaphore_wait(hello.at[2], 1))
            when(even, *c_c1[:OPEN])
        turn(late_m1, take_m1, k)
        turn(late_p1, take_p1, k)
        turn(late_c1, take_c1, k - LAG)

    c_own.wait_recv()
    s01 = colmax(sims(own2[...], own[...]))
    prior0 = jnp.maximum(prior0, jnp.where(c == 1, s01, neg))
    later0 = jnp.maximum(later0, jnp.where(c == 0, s01, neg))

    take_all(2, pc.at[0, 1 - c])

    def meet(a, kind, col):
        r = None
        for j in range(2):
            s = sims(a, pc[kind, j])
            col.append(colmax(s))
            r = lanes(s) if r is None else jnp.maximum(r, lanes(s))
        return r

    col0, col1, col2 = [], [], []
    r0 = meet(own[...], 0, col0)
    r1 = meet(m1[...], 0, col1)
    take_all(3, pc.at[1, 1 - c])
    r0 = jnp.maximum(r0, meet(own[...], 1, col0))
    r1 = jnp.maximum(r1, meet(m1[...], 1, col1))
    other = (c + h) % 2
    pblk, cblk = pc[0, c], pc[1, other]
    pcol = colmax(sims(cblk, pblk))
    ccol = colmax(sims(pblk, cblk))
    r0, r1 = flip(r0), flip(r1)

    for k in range(CHUNKS):
        c_e[k].wait_recv()
        n_e[k].start()
    take_all(0, m2)
    r2 = meet(m2[...], 0, col2)
    r2 = flip(jnp.maximum(r2, meet(m2[...], 1, col2)))
    ecol, re = [], None
    take_all(4, e.at[1 - c])
    for j in range(2):
        s = sims(m2[...], e[j])
        ecol.append(colmax(s))
        re = lanes(s) if re is None else jnp.maximum(re, lanes(s))
    re = flip(re)

    at = lambda dy: (y + dy + YS) % YS
    first0, first1, first2, first2e = at(0) < at(1), at(-1) < at(1), at(-2) < at(1), at(-2) < at(2)

    def pick(flag, v):
        return jnp.where(flag, v, neg)

    def top(*vs):
        o = vs[0]
        for v in vs[1:]:
            o = jnp.maximum(o, v)
        return o

    prior0 = top(prior0, pick(~first0, r0))
    later0 = top(later0, pick(first0, r0))

    def put(i, prior, later):
        msg_out[i, 0:1, :] = jnp.maximum(prior, neg)
        msg_out[i, 1:2, :] = jnp.maximum(later, neg)

    put(0, pick(~first1, r1), pick(first1, r1))
    put(1, top(pick(~first2, r2), pick(~first2e, re)), top(pick(first2, r2), pick(first2e, re)))
    for j in range(2):
        x = [col0[j], col1[j], col2[j]]
        mine = pick(c == j, pcol)
        put(2 + j,
            top(pick(h == 1, mine), *[pick(f, v) for f, v in zip((first0, first1, first2), x)]),
            top(pick(h == 0, mine), *[pick(~f, v) for f, v in zip((first0, first1, first2), x)]))
        x = [col0[2 + j], col1[2 + j], col2[2 + j]]
        mine = pick(other == j, ccol)
        put(4 + j,
            top(pick(h == 0, mine), *[pick(f, v) for f, v in zip((first0, first1, first2), x)]),
            top(pick(h == 1, mine), *[pick(~f, v) for f, v in zip((first0, first1, first2), x)]))
        put(6 + j, pick(first2e, ecol[j]), pick(~first2e, ecol[j]))

    put(8, prior0, later0)
    mine_out = pltpu.make_async_copy(msg_out.at[8], out.at[8], csem.at[0])
    mine_out.start()
    he = (h + ((y + 2) % YS) // 4) % 2
    for i, slot, d in [
        (0, 0, dev(-1, h, c)), (1, 1, dev(-2, h, c)),
        (2, 2 + c, dev(1, h, 0)), (3, 2 + c, dev(1, h, 1)),
        (4, 4 + c, dev(1, 1 - h, 0)), (5, 4 + c, dev(1, 1 - h, 1)),
        (6, 6 + c, dev(2, he, 0)), (7, 6 + c, dev(2, he, 1)),
    ]:
        copy(msg_out.at[i], out.at[slot], 9, r_all.at[5], d).start()
    copy(msg_out.at[0:8], out.at[0:8], 9, r_all.at[5], up).wait_recv()
    for stream in range(9):
        copy(own, m1, stream, r_all.at[0], up).wait_send()
    copy(msg_out.at[0:8], out.at[0:8], 9, r_all.at[5], up).wait_send()
    mine_out.wait()


def per_device(embeddings, doc_order):
    rows, width = embeddings.shape
    block = (rows, width)
    vm = lambda *lead: pltpu.VMEM((*lead, *block), jnp.bfloat16)
    dma = lambda *n: pltpu.SemaphoreType.DMA(n)
    both = pl.pallas_call(
        kernel,
        name="dedup",
        out_shape=jax.ShapeDtypeStruct((9, 2, rows), jnp.float32),
        in_specs=[pl.BlockSpec(memory_space=pltpu.HBM)] * 2,
        out_specs=pl.BlockSpec(memory_space=pl.ANY),
        scratch_shapes=[
            vm(), vm(), vm(), vm(2, 2), vm(2), vm(),
            pltpu.VMEM((1, rows), jnp.int32),
            pltpu.VMEM((9, 2, rows), jnp.float32),
            pltpu.SemaphoreType.REGULAR((4,)), dma(2), dma(10), dma(4, CHUNKS), dma(6),
        ],
        compiler_params=pltpu.CompilerParams(
            collective_id=0, has_side_effects=True
        ),
    )(embeddings, doc_order)
    return jnp.max(both[:, 0], axis=0), jnp.max(both[:, 1], axis=0)


def solution(mesh):
    return jax.shard_map(
        per_device,
        mesh=mesh,
        in_specs=(P(("clus", "seq"), None), P(("clus", "seq"), None)),
        out_specs=(P(("clus", "seq")), P(("clus", "seq"))),
        check_vma=False,
    )
```

```python
import jax
import jax.numpy as jnp
from jax import lax
from jax.experimental import pallas as pl
from jax.experimental.pallas import tpu as pltpu
from jax.sharding import PartitionSpec as P

MESH = pl.DeviceIdType.MESH
CHUNKS = 8
LAG = 5
OPEN = 2
DELTA = 2
YS = 8


def sims(left, right):
    return lax.dot_general(left, right, (((1,), (1,)), ((), ())), preferred_element_type=jnp.float32)


def colmax(s):
    return jnp.max(s, axis=0, keepdims=True)


def lanes(s):
    out = s[:, :128]
    for j in range(1, s.shape[1] // 128):
        out = jnp.maximum(out, s[:, j * 128 : (j + 1) * 128])
    return out


def flip(r):
    return jnp.max(jnp.transpose(r), axis=0, keepdims=True)


def kernel(emb, order, out, own, m1, m2, pc, e, own2, rank, msg_out,
           hello, csem, s_sem, r_ring, r_all):
    clus = lax.axis_index("clus")
    seq = lax.axis_index("seq")
    y, h, c = seq // 4, (seq // 2) % 2, seq % 2

    def dev(dy, hh, cc):
        return (clus, ((y + dy + YS) % YS) * 4 + hh * 2 + cc)

    up, down = dev(1, h, c), dev(-1, h, c)
    across, sib = dev(0, 1 - h, c), dev(0, h, 1 - c)
    rows = own.shape[0] // CHUNKS

    def part(k):
        return pl.ds(k * rows, rows)

    even = (y + h + c) % 2 == 0
    odd = jnp.logical_not(even)
    no = jnp.logical_not
    corner = (clus == 0) & (c == 0)
    late_m1 = corner & (h == 0) & (y == 1)
    late_p1 = corner & (h == 0) & (y == YS - 1)
    late_c1 = corner & (h == 1) & ((y == 0) | (y == YS - 1))

    def signal(sem, *devices):
        for d in devices:
            pl.semaphore_signal(sem, inc=1, device_id=d, device_id_type=MESH)

    barrier = pltpu.get_barrier_semaphore()
    load = pltpu.make_async_copy(emb, own, csem.at[0])
    load_rank = pltpu.make_async_copy(order, rank, csem.at[1])
    load.start()
    load_rank.start()
    pl.when(even)(lambda: signal(barrier, across, sib))
    pl.when(odd)(lambda: signal(barrier, up, down))

    @pl.when(even)
    def _():
        pl.semaphore_wait(barrier, 2)
        signal(hello.at[0], down)
        signal(hello.at[1], up)

    load.wait()

    def copy(src, dst, stream, r, d):
        return pltpu.make_async_remote_copy(
            src_ref=src, dst_ref=dst, send_sem=s_sem.at[stream], recv_sem=r, device_id=d, device_id_type=MESH
        )

    which = ((y + 1) % YS) // 4
    every = range(CHUNKS)
    c_m1 = [copy(own.at[part(k)], m1.at[part(k)], 0, r_ring.at[0, k], up) for k in every]
    c_p1 = [copy(own.at[part(k)], pc.at[0, c, part(k)], 1, r_ring.at[1, k], down) for k in every]
    c_m2 = [copy(m1.at[part(k)], m2.at[part(k)], 2, r_all.at[0], up) for k in every]
    c_e = [copy(pc.at[which, c, part(k)], e.at[c, part(k)], 3, r_ring.at[3, k], down) for k in every]
    c_c1 = [copy(pc.at[0, c, part(k)], pc.at[1, c, part(k)], 4, r_ring.at[2, k], across) for k in every]
    c_own = copy(own, own2, 5, r_all.at[1], sib)
    n_p1 = [copy(pc.at[0, c, part(k)], pc.at[0, c, part(k)], 6, r_all.at[2], sib) for k in every]
    n_c1 = [copy(pc.at[1, c, part(k)], pc.at[1, c, part(k)], 7, r_all.at[3], sib) for k in every]
    n_e = [copy(e.at[c, part(k)], e.at[c, part(k)], 8, r_all.at[4], sib) for k in every]

    def take_all(i, dst):
        copy(own, dst, 0, r_all.at[i], up).wait_recv()

    def when(flag, *copies):
        @pl.when(flag)
        def _():
            for one in copies:
                one.start()

    when(even, *[one for pair in zip(c_m1, c_p1) for one in pair])

    def open_up():
        pl.semaphore_wait(hello.at[0], 1)
        for one in c_m1:
            one.start()

    def open_down():
        pl.semaphore_wait(hello.at[1], 1)
        for one in c_p1:
            one.start()

    @pl.when(odd & (y < YS // 2))
    def _():
        open_up()
        open_down()

    @pl.when(odd & (y >= YS // 2))
    def _():
        open_down()
        open_up()

    load_rank.wait()

    neg = jnp.float32(-1.0)
    rank_cols = jnp.broadcast_to(rank[...].astype(jnp.float32), (256, 256))
    rank_rows = jnp.transpose(rank_cols)
    s = sims(own[...], own[...])
    prior0 = colmax(jnp.where(rank_rows < rank_cols, s, neg))
    later0 = colmax(jnp.where(rank_rows > rank_cols, s, neg))

    @pl.when(odd)
    def _():
        pl.semaphore_wait(barrier, 2)
        signal(hello.at[2], across)
        signal(hello.at[3], sib)

    pl.when(even)(lambda: pl.semaphore_wait(hello.at[3], 1))
    c_own.start()

    def take_m1(k):
        c_m1[k].wait_recv()
        c_m2[k].start()

    def take_p1(k):
        c_p1[k].wait_recv()
        if k < OPEN:
            when(odd, c_c1[k])
        else:
            c_c1[k].start()
        when(which == 0, c_e[k])
        n_p1[k].start()

    def take_c1(k):
        c_c1[k].wait_recv()
        when(which == 1, c_e[k])
        n_c1[k].start()

    def turn(late, take, k):
        if 0 <= k < CHUNKS:
            pl.when(no(late))(lambda: take(k))
        if 0 <= k - DELTA < CHUNKS:
            pl.when(late)(lambda: take(k - DELTA))

    def pick(flag, v):
        return jnp.where(flag, v, neg)

    def top(*vs):
        o = vs[0]
        for v in vs[1:]:
            o = jnp.maximum(o, v)
        return o

    def meet(a, blocks, col):
        r = None
        for j in range(2):
            s = sims(a, blocks[j, ...])
            col.append(colmax(s))
            r = lanes(s) if r is None else jnp.maximum(r, lanes(s))
        return r

    at = lambda dy: (y + dy + YS) % YS
    first0, first1, first2, first2e = at(0) < at(1), at(-1) < at(1), at(-2) < at(1), at(-2) < at(2)
    col0, col1, col2, ecol = [], [], [], []

    def near_products(prior0, later0):
        c_own.wait_recv()
        s01 = colmax(sims(own2[...], own[...]))
        prior0 = top(prior0, pick(c == 1, s01))
        later0 = top(later0, pick(c == 0, s01))
        take_all(2, pc.at[0, 1 - c])
        return prior0, later0, meet(own[...], pc.at[0], col0), meet(m1[...], pc.at[0], col1)

    for k in range(CHUNKS + LAG + DELTA):
        if k == CHUNKS + LAG + DELTA - 1:
            prior0, later0, r0, r1 = near_products(prior0, later0)
        if k == OPEN:
            pl.when(even)(lambda: pl.semaphore_wait(hello.at[2], 1))
            when(even, *c_c1[:OPEN])
        turn(late_m1, take_m1, k)
        turn(late_p1, take_p1, k)
        turn(late_c1, take_c1, k - LAG)

    take_all(3, pc.at[1, 1 - c])
    r0 = flip(top(r0, meet(own[...], pc.at[1], col0)))
    r1 = flip(top(r1, meet(m1[...], pc.at[1], col1)))
    other = (c + h) % 2
    pblk, cblk = pc[0, c], pc[1, other]
    pcol = colmax(sims(cblk, pblk))
    ccol = colmax(sims(pblk, cblk))
    for k in range(CHUNKS):
        c_e[k].wait_recv()
        n_e[k].start()

    def put(i, prior, later):
        msg_out[i, 0:1, :] = jnp.maximum(prior, neg)
        msg_out[i, 1:2, :] = jnp.maximum(later, neg)

    def post(i, slot, d):
        copy(msg_out.at[i], out.at[slot], 9, r_all.at[5], d).start()

    put(0, pick(~first1, r1), pick(first1, r1))
    put(8, top(prior0, pick(~first0, r0)), top(later0, pick(first0, r0)))
    post(0, 0, dev(-1, h, c))
    mine_out = pltpu.make_async_copy(msg_out.at[8], out.at[8], csem.at[0])
    mine_out.start()
    before, after = [], []
    for j in range(4):
        mine = pick(c == j, pcol) if j < 2 else pick(other == j - 2, ccol)
        home = h if j < 2 else 1 - h
        before.append(top(pick(home == 1, mine), pick(first0, col0[j]), pick(first1, col1[j])))
        after.append(top(pick(home == 0, mine), pick(~first0, col0[j]), pick(~first1, col1[j])))

    take_all(0, m2)
    r2 = meet(m2[...], pc.at[1], col2)
    for j in range(2):
        put(4 + j, top(before[2 + j], pick(first2, col2[j])), top(after[2 + j], pick(~first2, col2[j])))
    post(4, 4 + c, dev(1, 1 - h, 0))
    post(5, 4 + c, dev(1, 1 - h, 1))
    r2 = top(r2, meet(m2[...], pc.at[0], col2))
    take_all(4, e.at[1 - c])
    re = meet(m2[...], e, ecol)
    he = (h + ((y + 2) % YS) // 4) % 2
    for j in range(2):
        put(6 + j, pick(first2e, ecol[j]), pick(~first2e, ecol[j]))
    post(6, 6 + c, dev(2, he, 0))
    post(7, 6 + c, dev(2, he, 1))
    r2, re = flip(r2), flip(re)
    put(1, top(pick(~first2, r2), pick(~first2e, re)), top(pick(first2, r2), pick(first2e, re)))
    post(1, 1, dev(-2, h, c))
    for j in range(2):
        put(2 + j, top(before[j], pick(first2, col2[2 + j])), top(after[j], pick(~first2, col2[2 + j])))
    post(2, 2 + c, dev(1, h, 0))
    post(3, 2 + c, dev(1, h, 1))
    copy(msg_out.at[0:8], out.at[0:8], 9, r_all.at[5], up).wait_recv()
    for stream in range(9):
        copy(own, m1, stream, r_all.at[0], up).wait_send()
    copy(msg_out.at[0:8], out.at[0:8], 9, r_all.at[5], up).wait_send()
    mine_out.wait()


def per_device(embeddings, doc_order):
    rows, width = embeddings.shape
    block = (rows, width)
    vm = lambda *lead: pltpu.VMEM((*lead, *block), jnp.bfloat16)
    dma = lambda *n: pltpu.SemaphoreType.DMA(n)
    both = pl.pallas_call(
        kernel,
        name="dedup",
        out_shape=jax.ShapeDtypeStruct((9, 2, rows), jnp.float32),
        in_specs=[pl.BlockSpec(memory_space=pltpu.HBM)] * 2,
        out_specs=pl.BlockSpec(memory_space=pl.ANY),
        scratch_shapes=[
            vm(), vm(), vm(), vm(2, 2), vm(2), vm(),
            pltpu.VMEM((1, rows), jnp.int32),
            pltpu.VMEM((9, 2, rows), jnp.float32),
            pltpu.SemaphoreType.REGULAR((4,)), dma(2), dma(10), dma(4, CHUNKS), dma(6),
        ],
        compiler_params=pltpu.CompilerParams(
            collective_id=0, has_side_effects=True
        ),
    )(embeddings, doc_order)
    return jnp.max(both[:, 0], axis=0), jnp.max(both[:, 1], axis=0)


def solution(mesh):
    return jax.shard_map(
        per_device,
        mesh=mesh,
        in_specs=(P(("clus", "seq"), None), P(("clus", "seq"), None)),
        out_specs=(P(("clus", "seq")), P(("clus", "seq"))),
        check_vma=False,
    )
```

```python
import jax
import jax.numpy as jnp
from jax import lax
from jax.experimental import pallas as pl
from jax.experimental.pallas import tpu as pltpu
from jax.sharding import PartitionSpec as P

MESH = pl.DeviceIdType.MESH
CHUNKS = 8
LAG = 5
OPEN = 2
DELTA = 2
YS = 8


def sims(left, right):
    return lax.dot_general(left, right, (((1,), (1,)), ((), ())), preferred_element_type=jnp.float32)


def colmax(s):
    return jnp.max(s, axis=0, keepdims=True)


def lanes(s):
    out = s[:, :128]
    for j in range(1, s.shape[1] // 128):
        out = jnp.maximum(out, s[:, j * 128 : (j + 1) * 128])
    return out


def flip(r):
    return jnp.max(jnp.transpose(r), axis=0, keepdims=True)


def kernel(emb, order, out, own, m1, m2, pc, e, own2, rank, msg_out,
           hello, csem, s_sem, r_ring, r_all):
    clus = lax.axis_index("clus")
    seq = lax.axis_index("seq")
    y, h, c = seq // 4, (seq // 2) % 2, seq % 2

    def dev(dy, hh, cc):
        return (clus, ((y + dy + YS) % YS) * 4 + hh * 2 + cc)

    up, down = dev(1, h, c), dev(-1, h, c)
    across, sib = dev(0, 1 - h, c), dev(0, h, 1 - c)
    rows = own.shape[0] // CHUNKS

    def part(k):
        return pl.ds(k * rows, rows)

    even = (y + h + c) % 2 == 0
    odd = jnp.logical_not(even)
    no = jnp.logical_not
    corner = (clus == 0) & (c == 0)
    late_m1 = corner & (h == 0) & (y == 1)
    late_p1 = corner & (h == 0) & (y == YS - 1)
    late_c1 = corner & (h == 1) & ((y == 0) | (y == YS - 1))

    def signal(sem, *devices):
        for d in devices:
            pl.semaphore_signal(sem, inc=1, device_id=d, device_id_type=MESH)

    barrier = pltpu.get_barrier_semaphore()
    load = pltpu.make_async_copy(emb, own, csem.at[0])
    load_rank = pltpu.make_async_copy(order, rank, csem.at[1])
    load.start()
    load_rank.start()
    pl.when(even)(lambda: signal(barrier, across, sib))
    pl.when(odd)(lambda: signal(barrier, up, down))

    @pl.when(even)
    def _():
        pl.semaphore_wait(barrier, 2)
        signal(hello.at[0], down)
        signal(hello.at[1], up)

    load.wait()

    def copy(src, dst, stream, r, d):
        return pltpu.make_async_remote_copy(
            src_ref=src, dst_ref=dst, send_sem=s_sem.at[stream], recv_sem=r, device_id=d, device_id_type=MESH
        )

    which = ((y + 1) % YS) // 4
    every = range(CHUNKS)
    c_m1 = [copy(own.at[part(k)], m1.at[part(k)], 0, r_ring.at[0, k], up) for k in every]
    c_p1 = [copy(own.at[part(k)], pc.at[0, c, part(k)], 1, r_ring.at[1, k], down) for k in every]
    c_m2 = [copy(m1.at[part(k)], m2.at[part(k)], 2, r_all.at[0], up) for k in every]
    c_e = [copy(pc.at[which, c, part(k)], e.at[c, part(k)], 3, r_ring.at[3, k], down) for k in every]
    c_c1 = [copy(pc.at[0, c, part(k)], pc.at[1, c, part(k)], 4, r_ring.at[2, k], across) for k in every]
    c_own = copy(own, own2, 5, r_all.at[1], sib)
    n_p1 = [copy(pc.at[0, c, part(k)], pc.at[0, c, part(k)], 6, r_all.at[2], sib) for k in every]
    n_c1 = [copy(pc.at[1, c, part(k)], pc.at[1, c, part(k)], 7, r_all.at[3], sib) for k in every]
    n_e = [copy(e.at[c, part(k)], e.at[c, part(k)], 8, r_all.at[4], sib) for k in every]

    def take_all(i, dst):
        copy(own, dst, 0, r_all.at[i], up).wait_recv()

    def when(flag, *copies):
        @pl.when(flag)
        def _():
            for one in copies:
                one.start()

    when(even, *[one for pair in zip(c_m1, c_p1) for one in pair])

    def open_up():
        pl.semaphore_wait(hello.at[0], 1)
        for one in c_m1:
            one.start()

    def open_down():
        pl.semaphore_wait(hello.at[1], 1)
        for one in c_p1:
            one.start()

    @pl.when(odd & (y <= YS // 2))
    def _():
        open_up()
        open_down()

    @pl.when(odd & (y > YS // 2))
    def _():
        open_down()
        open_up()

    load_rank.wait()

    neg = jnp.float32(-1.0)
    rank_cols = jnp.broadcast_to(rank[...].astype(jnp.float32), (256, 256))
    rank_rows = jnp.transpose(rank_cols)
    s = sims(own[...], own[...])
    prior0 = colmax(jnp.where(rank_rows < rank_cols, s, neg))
    later0 = colmax(jnp.where(rank_rows > rank_cols, s, neg))

    @pl.when(odd)
    def _():
        pl.semaphore_wait(barrier, 2)
        signal(hello.at[2], across)
        signal(hello.at[3], sib)

    pl.when(even)(lambda: pl.semaphore_wait(hello.at[3], 1))
    c_own.start()

    def take_m1(k):
        c_m1[k].wait_recv()
        c_m2[k].start()

    def take_p1(k):
        c_p1[k].wait_recv()
        if k < OPEN:
            when(odd, c_c1[k])
        else:
            c_c1[k].start()
        when(which == 0, c_e[k])
        n_p1[k].start()

    def take_c1(k):
        c_c1[k].wait_recv()
        when(which == 1, c_e[k])
        n_c1[k].start()

    def turn(late, take, k):
        if 0 <= k < CHUNKS:
            pl.when(no(late))(lambda: take(k))
        if 0 <= k - DELTA < CHUNKS:
            pl.when(late)(lambda: take(k - DELTA))

    def pick(flag, v):
        return jnp.where(flag, v, neg)

    def top(*vs):
        o = vs[0]
        for v in vs[1:]:
            o = jnp.maximum(o, v)
        return o

    def meet(a, blocks, col):
        r = None
        for j in range(2):
            s = sims(a, blocks[j, ...])
            col.append(colmax(s))
            r = lanes(s) if r is None else jnp.maximum(r, lanes(s))
        return r

    at = lambda dy: (y + dy + YS) % YS
    first0, first1, first2, first2e = at(0) < at(1), at(-1) < at(1), at(-2) < at(1), at(-2) < at(2)
    col0, col1, col2, ecol = [], [], [], []

    def near_products(prior0, later0):
        c_own.wait_recv()
        s01 = colmax(sims(own2[...], own[...]))
        prior0 = top(prior0, pick(c == 1, s01))
        later0 = top(later0, pick(c == 0, s01))
        take_all(2, pc.at[0, 1 - c])
        return prior0, later0, meet(own[...], pc.at[0], col0), meet(m1[...], pc.at[0], col1)

    for k in range(CHUNKS + LAG + DELTA):
        if k == CHUNKS + LAG + DELTA - 1:
            prior0, later0, r0, r1 = near_products(prior0, later0)
        if k == OPEN:
            pl.when(even)(lambda: pl.semaphore_wait(hello.at[2], 1))
            when(even, *c_c1[:OPEN])
        turn(late_m1, take_m1, k)
        turn(late_p1, take_p1, k)
        turn(late_c1, take_c1, k - LAG)

    take_all(3, pc.at[1, 1 - c])
    r0 = flip(top(r0, meet(own[...], pc.at[1], col0)))
    r1 = flip(top(r1, meet(m1[...], pc.at[1], col1)))
    other = (c + h) % 2
    pblk, cblk = pc[0, c], pc[1, other]
    pcol = colmax(sims(cblk, pblk))
    ccol = colmax(sims(pblk, cblk))
    for k in range(CHUNKS):
        c_e[k].wait_recv()
        n_e[k].start()

    def put(i, prior, later):
        msg_out[i, 0:1, :] = jnp.maximum(prior, neg)
        msg_out[i, 1:2, :] = jnp.maximum(later, neg)

    def post(i, slot, d):
        copy(msg_out.at[i], out.at[slot], 9, r_all.at[5], d).start()

    put(0, pick(~first1, r1), pick(first1, r1))
    put(8, top(prior0, pick(~first0, r0)), top(later0, pick(first0, r0)))
    post(0, 0, dev(-1, h, c))
    mine_out = pltpu.make_async_copy(msg_out.at[8], out.at[8], csem.at[0])
    mine_out.start()
    before, after = [], []
    for j in range(4):
        mine = pick(c == j, pcol) if j < 2 else pick(other == j - 2, ccol)
        home = h if j < 2 else 1 - h
        before.append(top(pick(home == 1, mine), pick(first0, col0[j]), pick(first1, col1[j])))
        after.append(top(pick(home == 0, mine), pick(~first0, col0[j]), pick(~first1, col1[j])))

    take_all(0, m2)
    r2 = meet(m2[...], pc.at[1], col2)
    for j in range(2):
        put(4 + j, top(before[2 + j], pick(first2, col2[j])), top(after[2 + j], pick(~first2, col2[j])))
    post(4, 4 + c, dev(1, 1 - h, 0))
    post(5, 4 + c, dev(1, 1 - h, 1))
    r2 = top(r2, meet(m2[...], pc.at[0], col2))
    take_all(4, e.at[1 - c])
    re = meet(m2[...], e, ecol)
    he = (h + ((y + 2) % YS) // 4) % 2
    for j in range(2):
        put(6 + j, pick(first2e, ecol[j]), pick(~first2e, ecol[j]))
    post(6, 6 + c, dev(2, he, 0))
    post(7, 6 + c, dev(2, he, 1))
    r2, re = flip(r2), flip(re)
    put(1, top(pick(~first2, r2), pick(~first2e, re)), top(pick(first2, r2), pick(first2e, re)))
    post(1, 1, dev(-2, h, c))
    for j in range(2):
        put(2 + j, top(before[j], pick(first2, col2[2 + j])), top(after[j], pick(~first2, col2[2 + j])))
    post(2, 2 + c, dev(1, h, 0))
    post(3, 2 + c, dev(1, h, 1))
    copy(msg_out.at[0:8], out.at[0:8], 9, r_all.at[5], up).wait_recv()
    for stream in range(9):
        copy(own, m1, stream, r_all.at[0], up).wait_send()
    copy(msg_out.at[0:8], out.at[0:8], 9, r_all.at[5], up).wait_send()
    mine_out.wait()


def per_device(embeddings, doc_order):
    rows, width = embeddings.shape
    block = (rows, width)
    vm = lambda *lead: pltpu.VMEM((*lead, *block), jnp.bfloat16)
    dma = lambda *n: pltpu.SemaphoreType.DMA(n)
    both = pl.pallas_call(
        kernel,
        name="dedup",
        out_shape=jax.ShapeDtypeStruct((9, 2, rows), jnp.float32),
        in_specs=[pl.BlockSpec(memory_space=pltpu.HBM)] * 2,
        out_specs=pl.BlockSpec(memory_space=pl.ANY),
        scratch_shapes=[
            vm(), vm(), vm(), vm(2, 2), vm(2), vm(),
            pltpu.VMEM((1, rows), jnp.int32),
            pltpu.VMEM((9, 2, rows), jnp.float32),
            pltpu.SemaphoreType.REGULAR((4,)), dma(2), dma(10), dma(4, CHUNKS), dma(6),
        ],
        compiler_params=pltpu.CompilerParams(
            collective_id=0, has_side_effects=True, vmem_limit_bytes=55000 * 1024
        ),
    )(
        pltpu.with_memory_space_constraint(embeddings, pltpu.HBM),
        pltpu.with_memory_space_constraint(doc_order, pltpu.HBM),
    )
    return jnp.max(both[:, 0], axis=0), jnp.max(both[:, 1], axis=0)


def solution(mesh):
    return jax.shard_map(
        per_device,
        mesh=mesh,
        in_specs=(P(("clus", "seq"), None), P(("clus", "seq"), None)),
        out_specs=(P(("clus", "seq")), P(("clus", "seq"))),
        check_vma=False,
    )
```

```python
import jax
import jax.numpy as jnp
from jax import lax
from jax.experimental import pallas as pl
from jax.experimental.pallas import tpu as pltpu
from jax.sharding import PartitionSpec as P

MESH = pl.DeviceIdType.MESH
CHUNKS = 8
LAG = 5
OPEN = 1
DELTA = 3
YS = 8


def sims(left, right):
    return lax.dot_general(left, right, (((1,), (1,)), ((), ())), preferred_element_type=jnp.float32)


def colmax(s):
    return jnp.max(s, axis=0, keepdims=True)


def lanes(s):
    out = s[:, :128]
    for j in range(1, s.shape[1] // 128):
        out = jnp.maximum(out, s[:, j * 128 : (j + 1) * 128])
    return out


def flip(r):
    return jnp.max(jnp.transpose(r), axis=0, keepdims=True)


def kernel(emb, order, out, own, m1, m2, pc, e, own2, rank, msg_out,
           hello, csem, s_sem, r_ring, r_all):
    clus = lax.axis_index("clus")
    seq = lax.axis_index("seq")
    y, h, c = seq // 4, (seq // 2) % 2, seq % 2

    def dev(dy, hh, cc):
        return (clus, ((y + dy + YS) % YS) * 4 + hh * 2 + cc)

    up, down = dev(1, h, c), dev(-1, h, c)
    across, sib = dev(0, 1 - h, c), dev(0, h, 1 - c)
    rows = own.shape[0] // CHUNKS

    def part(k):
        return pl.ds(k * rows, rows)

    even = (y + h + c) % 2 == 0
    odd = jnp.logical_not(even)
    no = jnp.logical_not
    corner = (clus == 0) & (c == 0)
    late_m1 = corner & (h == 0) & (y == 1)
    late_p1 = corner & (h == 0) & (y == YS - 1)
    slow = (clus == 0) & ((y == 0) | (y == YS - 1))
    late_c1 = corner & (h == 1) & ((y == 0) | (y == YS - 1))

    def signal(sem, *devices):
        for d in devices:
            pl.semaphore_signal(sem, inc=1, device_id=d, device_id_type=MESH)

    barrier = pltpu.get_barrier_semaphore()
    load = pltpu.make_async_copy(emb, own, csem.at[0])
    load_rank = pltpu.make_async_copy(order, rank, csem.at[1])
    load.start()
    load_rank.start()
    pl.when(even)(lambda: signal(barrier, across, sib))
    pl.when(odd)(lambda: signal(barrier, up, down))

    @pl.when(even)
    def _():
        pl.semaphore_wait(barrier, 2)
        signal(hello.at[0], down)
        signal(hello.at[1], up)

    load.wait()

    def copy(src, dst, stream, r, d):
        return pltpu.make_async_remote_copy(
            src_ref=src, dst_ref=dst, send_sem=s_sem.at[stream], recv_sem=r, device_id=d, device_id_type=MESH
        )

    which = ((y + 1) % YS) // 4
    every = range(CHUNKS)
    c_m1 = [copy(own.at[part(k)], m1.at[part(k)], 0, r_ring.at[0, k], up) for k in every]
    c_p1 = [copy(own.at[part(k)], pc.at[0, c, part(k)], 1, r_ring.at[1, k], down) for k in every]
    c_m2 = [copy(m1.at[part(k)], m2.at[part(k)], 2, r_all.at[0], up) for k in every]
    c_e = [copy(pc.at[which, c, part(k)], e.at[c, part(k)], 3, r_ring.at[3, k], down) for k in every]
    c_c1 = [copy(pc.at[0, c, part(k)], pc.at[1, c, part(k)], 4, r_ring.at[2, k], across) for k in every]
    c_own = copy(own, own2, 5, r_all.at[1], sib)
    n_p1 = [copy(pc.at[0, c, part(k)], pc.at[0, c, part(k)], 6, r_all.at[2], sib) for k in every]
    n_c1 = [copy(pc.at[1, c, part(k)], pc.at[1, c, part(k)], 7, r_all.at[3], sib) for k in every]
    n_e = [copy(e.at[c, part(k)], e.at[c, part(k)], 8, r_all.at[4], sib) for k in every]

    def take_all(i, dst):
        copy(own, dst, 0, r_all.at[i], up).wait_recv()

    def when(flag, *copies):
        @pl.when(flag)
        def _():
            for one in copies:
                one.start()

    when(even, *[one for pair in zip(c_m1, c_p1) for one in pair])

    def open_up():
        pl.semaphore_wait(hello.at[0], 1)
        for one in c_m1:
            one.start()

    def open_down():
        pl.semaphore_wait(hello.at[1], 1)
        for one in c_p1:
            one.start()

    @pl.when(odd & (y <= YS // 2))
    def _():
        open_up()
        open_down()

    @pl.when(odd & (y > YS // 2))
    def _():
        open_down()
        open_up()

    load_rank.wait()

    neg = jnp.float32(-1.0)
    rank_cols = jnp.broadcast_to(rank[...].astype(jnp.float32), (256, 256))
    rank_rows = jnp.transpose(rank_cols)
    s = sims(own[...], own[...])
    prior0 = colmax(jnp.where(rank_rows < rank_cols, s, neg))
    later0 = colmax(jnp.where(rank_rows > rank_cols, s, neg))

    @pl.when(odd)
    def _():
        pl.semaphore_wait(barrier, 2)
        signal(hello.at[2], across)
        signal(hello.at[3], sib)

    pl.when(even)(lambda: pl.semaphore_wait(hello.at[3], 1))
    c_own.start()

    def take_m1(k):
        c_m1[k].wait_recv()
        c_m2[k].start()

    def take_p1(k):
        c_p1[k].wait_recv()
        if k < OPEN:
            when(odd, c_c1[k])
        else:
            c_c1[k].start()
        when(which == 0, c_e[k])
        n_p1[k].start()

    def take_c1(k):
        c_c1[k].wait_recv()
        when(which == 1, c_e[k])
        n_c1[k].start()

    def turn(late, take, k):
        if 0 <= k < CHUNKS:
            pl.when(no(late))(lambda: take(k))
        if 0 <= k - DELTA < CHUNKS:
            pl.when(late)(lambda: take(k - DELTA))

    def pick(flag, v):
        return jnp.where(flag, v, neg)

    def top(*vs):
        o = vs[0]
        for v in vs[1:]:
            o = jnp.maximum(o, v)
        return o

    def meet(a, blocks, col):
        r = None
        for j in range(2):
            s = sims(a, blocks[j, ...])
            col.append(colmax(s))
            r = lanes(s) if r is None else jnp.maximum(r, lanes(s))
        return r

    at = lambda dy: (y + dy + YS) % YS
    first0, first1, first2, first2e = at(0) < at(1), at(-1) < at(1), at(-2) < at(1), at(-2) < at(2)
    col0, col1, col2, ecol = [], [], [], []

    def near_products(prior0, later0):
        c_own.wait_recv()
        s01 = colmax(sims(own2[...], own[...]))
        prior0 = top(prior0, pick(c == 1, s01))
        later0 = top(later0, pick(c == 0, s01))
        take_all(2, pc.at[0, 1 - c])
        return prior0, later0, meet(own[...], pc.at[0], col0), meet(m1[...], pc.at[0], col1)

    for k in range(CHUNKS + LAG + DELTA):
        if k == CHUNKS + LAG + DELTA - 1:
            prior0, later0, r0, r1 = near_products(prior0, later0)
        if k == OPEN:
            pl.when(even)(lambda: pl.semaphore_wait(hello.at[2], 1))
            when(even, *c_c1[:OPEN])
        turn(late_m1, take_m1, k)
        turn(late_p1, take_p1, k)
        if 0 <= k - LAG + 1 < CHUNKS:
            pl.when(no(slow))(lambda: take_c1(k - LAG + 1))
        if 0 <= k - LAG < CHUNKS:
            pl.when(slow & no(late_c1))(lambda: take_c1(k - LAG))
        if 0 <= k - LAG - DELTA < CHUNKS:
            pl.when(late_c1)(lambda: take_c1(k - LAG - DELTA))

    take_all(3, pc.at[1, 1 - c])
    r0 = flip(top(r0, meet(own[...], pc.at[1], col0)))
    r1 = flip(top(r1, meet(m1[...], pc.at[1], col1)))
    other = (c + h) % 2
    pblk, cblk = pc[0, c], pc[1, other]
    pcol = colmax(sims(cblk, pblk))
    ccol = colmax(sims(pblk, cblk))
    for k in range(CHUNKS):
        c_e[k].wait_recv()
        n_e[k].start()

    def put(i, prior, later):
        msg_out[i, 0:1, :] = jnp.maximum(prior, neg)
        msg_out[i, 1:2, :] = jnp.maximum(later, neg)

    def post(i, slot, d):
        copy(msg_out.at[i], out.at[slot], 9, r_all.at[5], d).start()

    put(0, pick(~first1, r1), pick(first1, r1))
    put(8, top(prior0, pick(~first0, r0)), top(later0, pick(first0, r0)))
    post(0, 0, dev(-1, h, c))
    mine_out = pltpu.make_async_copy(msg_out.at[8], out.at[8], csem.at[0])
    mine_out.start()
    before, after = [], []
    for j in range(4):
        mine = pick(c == j, pcol) if j < 2 else pick(other == j - 2, ccol)
        home = h if j < 2 else 1 - h
        before.append(top(pick(home == 1, mine), pick(first0, col0[j]), pick(first1, col1[j])))
        after.append(top(pick(home == 0, mine), pick(~first0, col0[j]), pick(~first1, col1[j])))

    take_all(0, m2)
    r2 = meet(m2[...], pc.at[1], col2)
    for j in range(2):
        put(4 + j, top(before[2 + j], pick(first2, col2[j])), top(after[2 + j], pick(~first2, col2[j])))
    post(4, 4 + c, dev(1, 1 - h, 0))
    post(5, 4 + c, dev(1, 1 - h, 1))
    r2 = top(r2, meet(m2[...], pc.at[0], col2))
    take_all(4, e.at[1 - c])
    re = meet(m2[...], e, ecol)
    he = (h + ((y + 2) % YS) // 4) % 2
    for j in range(2):
        put(6 + j, pick(first2e, ecol[j]), pick(~first2e, ecol[j]))
    post(6, 6 + c, dev(2, he, 0))
    post(7, 6 + c, dev(2, he, 1))
    r2, re = flip(r2), flip(re)
    put(1, top(pick(~first2, r2), pick(~first2e, re)), top(pick(first2, r2), pick(first2e, re)))
    post(1, 1, dev(-2, h, c))
    for j in range(2):
        put(2 + j, top(before[j], pick(first2, col2[2 + j])), top(after[j], pick(~first2, col2[2 + j])))
    post(2, 2 + c, dev(1, h, 0))
    post(3, 2 + c, dev(1, h, 1))
    copy(msg_out.at[0:8], out.at[0:8], 9, r_all.at[5], up).wait_recv()
    for stream in range(9):
        copy(own, m1, stream, r_all.at[0], up).wait_send()
    copy(msg_out.at[0:8], out.at[0:8], 9, r_all.at[5], up).wait_send()
    mine_out.wait()


def per_device(embeddings, doc_order):
    rows, width = embeddings.shape
    block = (rows, width)
    vm = lambda *lead: pltpu.VMEM((*lead, *block), jnp.bfloat16)
    dma = lambda *n: pltpu.SemaphoreType.DMA(n)
    both = pl.pallas_call(
        kernel,
        name="dedup",
        out_shape=jax.ShapeDtypeStruct((9, 2, rows), jnp.float32),
        in_specs=[pl.BlockSpec(memory_space=pltpu.HBM)] * 2,
        out_specs=pl.BlockSpec(memory_space=pl.ANY),
        scratch_shapes=[
            vm(), vm(), vm(), vm(2, 2), vm(2), vm(),
            pltpu.VMEM((1, rows), jnp.int32),
            pltpu.VMEM((9, 2, rows), jnp.float32),
            pltpu.SemaphoreType.REGULAR((4,)), dma(2), dma(10), dma(4, CHUNKS), dma(6),
        ],
        compiler_params=pltpu.CompilerParams(
            collective_id=0, has_side_effects=True, vmem_limit_bytes=55000 * 1024
        ),
    )(
        pltpu.with_memory_space_constraint(embeddings, pltpu.HBM),
        pltpu.with_memory_space_constraint(doc_order, pltpu.HBM),
    )
    return jnp.max(both[:, 0], axis=0), jnp.max(both[:, 1], axis=0)


def solution(mesh):
    return jax.shard_map(
        per_device,
        mesh=mesh,
        in_specs=(P(("clus", "seq"), None), P(("clus", "seq"), None)),
        out_specs=(P(("clus", "seq")), P(("clus", "seq"))),
        check_vma=False,
    )
```
